32 devices in a mesh: dp: 8 (over z, x), mp: 4 (over y, core).
Axes of the slice: x: 2, y: 2, z: 4, core: 2. Of those that a mesh axis runs over, the one named last changes fastest.
Arguments:
- vlm_tokens: bfloat16 [2048, 2048], P(('dp', 'mp')), may hold values from -64 to 64
- action_tokens: bfloat16 [4096, 2048], P(('dp', 'mp')), may hold values from -64 to 64
- norm_gain: float32 [2048], replicated, may hold values from 0.25 to 1.75
- proj_old: bfloat16 [4096, 4096], P('dp', 'mp'), may hold values from -0.125 to 0.125
Outputs:
- vlm_hidden: bfloat16 [4096, 4096], P('dp', 'mp')
- action_hidden: bfloat16 [4096, 8192], P('dp', 'mp')
- proj_new: bfloat16 [2048, 8192], P('dp', 'mp')
The draws below stay inside these ranges and needn't reach their ends.
All inputs are finite; a program needn't handle non-finite values.
Results may differ from the reference program's by a relative error of at most 0.005.
Values may be sent and summed in bfloat16 or wider, within the bound.
A program may use at most 64 MiB of HBM per device.

```python
import math
import jax
import jax.numpy as jnp
from jax import lax

D = 2048
FF = 8192
VLM_TOK = 512
ACT_TOK = 512
VLM_ALL = 2048
ACT_ALL = 4096
N_DP = 8
N_MP = 4


def make_tokens(key, number_rows):
    key_base, key_column, key_row = jax.random.split(key, 3)
    entries = jax.random.normal(key_base, (number_rows, D), jnp.float32)
    column = jnp.exp(jax.random.uniform(key_column, (1, D), jnp.float32, math.log(0.3), math.log(3.0)))
    row_scale = jnp.exp(jax.random.uniform(key_row, (number_rows, 1), jnp.float32, 0.0, math.log(10.0)))
    return jnp.clip(entries * column * row_scale, -64.0, 64.0).astype(jnp.bfloat16)


def draw_vlm_tokens(key, part):
    return make_tokens(jax.random.fold_in(key, 11), VLM_ALL)


def draw_action_tokens(key, part):
    return make_tokens(jax.random.fold_in(key, 23), ACT_ALL)


def levels(key, dims, shards, low, top_value):
    level, own = 1.0, jax.random.fold_in(key, 6)
    for dim, parts in shards:
        heights = jnp.exp(jax.random.uniform(jax.random.fold_in(own, dim), (parts,), jnp.float32, low / len(shards), top_value / len(shards)))
        level = level * jnp.repeat(heights, dims[dim] // parts).reshape([-1 if axis == dim else 1 for axis in range(len(dims))])
    return level


def gaussian(key, dims, width, most, cuts=(), kind=jnp.bfloat16):
    factor_of = levels(key, dims, cuts, -0.22, 0.18) if cuts else 1.0
    values = jax.random.normal(key, dims, jnp.float32) * width * factor_of
    return jnp.minimum(jnp.maximum(values, -most), most).astype(kind)


def setup_inputs(seed: int = 0) -> dict:
    key_list = jax.random.split(jax.random.key(seed), 5)
    vlm_tokens = draw_vlm_tokens(jax.random.fold_in(key_list[4], 71), 0)
    action_tokens = draw_action_tokens(jax.random.fold_in(key_list[4], 71), 0)
    norm_gain = jnp.clip(1.0 + 0.15 * jax.random.normal(key_list[2], (D,), jnp.float32), 0.25, 1.75)
    proj_old = gaussian(key_list[3], (2 * D, FF // 2), D ** -0.5, 0.125, ((0, 8), (1, 4)))
    return dict(vlm_tokens=vlm_tokens, action_tokens=action_tokens, norm_gain=norm_gain, proj_old=proj_old)


epsilon = 1e-06

def normalize(row_values, norm_gain):
    values = row_values.astype(jnp.float32)
    factor = lax.rsqrt(lax.optimization_barrier(jnp.mean(values * values, axis=-1, keepdims=True)) + epsilon)
    return (values * factor * norm_gain).astype(jnp.bfloat16)

def reference(vlm_tokens, action_tokens, norm_gain, proj_old):
    groups = N_DP // 2
    row_block = 2 * D // N_DP
    col_block = FF // (2 * N_MP)
    weight = proj_old.reshape(groups, 2, row_block, N_MP, col_block).transpose(0, 2, 3, 1, 4).reshape(D, FF)

    def forward(tokens_block):
        normed = normalize(tokens_block, norm_gain)
        product = jnp.dot(normed, weight, preferred_element_type=jnp.float32)
        return jax.nn.gelu(product, approximate=False).astype(jnp.bfloat16)
    hidden_vlm = lax.map(forward, vlm_tokens.reshape(groups, VLM_TOK, D))
    vlm_hidden = hidden_vlm.reshape(groups, VLM_TOK, N_MP, 2, col_block).transpose(0, 3, 1, 2, 4).reshape(2 * VLM_ALL, FF // 2)
    action_hidden = lax.map(forward, action_tokens.reshape(N_DP, ACT_TOK, D)).reshape(ACT_ALL, FF)
    return (vlm_hidden, action_hidden, weight)
```

```python
import functools
import math
import jax
import jax.numpy as jnp
from jax import lax
from jax.experimental import pallas as pl
from jax.experimental.pallas import tpu as pltpu
from jax.sharding import PartitionSpec as P

MESH = pl.DeviceIdType.MESH
epsilon = 1e-06
CHUNKS = 4


def normalize(row_values, norm_gain):
    values = row_values.astype(jnp.float32)
    factor = lax.rsqrt(jnp.mean(values * values, axis=-1, keepdims=True) + epsilon)
    return (values * factor * norm_gain).astype(jnp.bfloat16)


def gelu(u):
    return (u * 0.5 * (1.0 + lax.erf(u * math.sqrt(0.5)))).astype(jnp.bfloat16)


def kernel(groups, mp_size, chunks, vlm_ref, act_ref, gain_ref, proj_ref, vlm_out, act_out, new_out,
           tok, wbuf, hid, tok_send, tok_recv, w_send, w_recv, ex_send, ex_recv, hid_send, hid_recv, loc):
    d = lax.axis_index("dp")
    m = lax.axis_index("mp")
    g, p = d // 2, d % 2
    y, c = m // 2, m % 2
    vr, ar = vlm_ref.shape[0], act_ref.shape[0]
    r, cols = proj_ref.shape
    half = r // 2
    cw = cols // chunks
    vlm_rows, act_rows = 2 * mp_size * vr, mp_size * ar
    sibling = (d, y * 2 + 1 - c)
    xpart = (g * 2 + 1 - p, m)
    ypart = (d, (1 - y) * 2 + c)
    has_left, has_right = g > 0, g < groups - 1

    barrier = pltpu.get_barrier_semaphore()
    for other in (sibling, xpart, ypart):
        pl.semaphore_signal(barrier, inc=1, device_id=other, device_id_type=MESH)

    @pl.when(has_left)
    def _():
        pl.semaphore_signal(barrier, inc=1, device_id=(d - 2, m), device_id_type=MESH)

    @pl.when(has_right)
    def _():
        pl.semaphore_signal(barrier, inc=1, device_id=(d + 2, m), device_id_type=MESH)

    def load_w():
        return pltpu.make_async_copy(proj_ref, wbuf.at[pl.ds(pl.multiple_of(g * r, r), r), :], loc.at[0])

    load_w().start()

    def place(pp, mm):
        s = pp * mp_size + mm
        return (pl.ds(pl.multiple_of(s * vr, vr), vr), pl.ds(pl.multiple_of(vlm_rows + s * ar, ar), ar), s)

    step = 32
    v0, a0, _ = place(p, m)

    @pl.loop(0, vr // step)
    def _(i):
        o = pl.multiple_of(i * step, step)
        tok[pl.ds(pl.multiple_of((p * mp_size + m) * vr + o, step), step), :] = normalize(
            vlm_ref[pl.ds(o, step), :], gain_ref[...])

    @pl.loop(0, ar // step)
    def _(i):
        o = pl.multiple_of(i * step, step)
        tok[pl.ds(pl.multiple_of(vlm_rows + (p * mp_size + m) * ar + o, step), step), :] = normalize(
            act_ref[pl.ds(o, step), :], gain_ref[...])

    pl.semaphore_wait(barrier, 3 + has_left.astype(jnp.int32) + has_right.astype(jnp.int32))

    def w_copy(block, k, side, own=False):
        rows = pl.ds(pl.multiple_of(block * r, r), r)
        cc = pl.ds(pl.multiple_of(k * cw, cw), cw)
        return pltpu.make_async_remote_copy(
            src_ref=proj_ref.at[:, cc] if own else wbuf.at[rows, cc],
            dst_ref=wbuf.at[rows, cc],
            send_sem=w_send.at[side, block, k],
            recv_sem=w_recv.at[block, k],
            device_id=(d - 2 if side == 0 else d + 2, m),
            device_id_type=MESH,
        )

    def send_w(block, k, own=False):
        @pl.when(has_left & (block >= g))
        def _():
            w_copy(block, k, 0, own).start()

        @pl.when(has_right & (block <= g))
        def _():
            w_copy(block, k, 1, own).start()

    for k in range(chunks):
        send_w(g, k, True)

    def tok_copies(pp, mm, to, slot):
        va, aa, s = place(pp, mm)
        return [pltpu.make_async_remote_copy(
            src_ref=tok.at[rows, :], dst_ref=tok.at[rows, :], send_sem=tok_send.at[slot, j],
            recv_sem=tok_recv.at[s, j], device_id=to, device_id_type=MESH)
            for j, rows in enumerate((va, aa))]

    def tok_start(pp, mm, to, slot):
        for copy in tok_copies(pp, mm, to, slot):
            copy.start()

    def tok_arrive(pp, mm):
        for copy in tok_copies(pp, mm, sibling, 0):
            copy.wait_recv()

    m_y = (1 - y) * 2 + c
    m_s = y * 2 + 1 - c
    m_ys = (1 - y) * 2 + 1 - c
    tok_start(p, m, xpart, 0)
    tok_start(p, m, ypart, 1)
    tok_start(p, m, sibling, 2)

    given = pl.multiple_of((1 - p) * half, half)
    ex = pltpu.make_async_remote_copy(
        src_ref=proj_ref.at[pl.ds(given, half), :],
        dst_ref=new_out.at[:, pl.ds(pl.multiple_of(p * cols, cols), cols)],
        send_sem=ex_send, recv_sem=ex_recv, device_id=xpart, device_id_type=MESH)
    ex.start()
    load_w().wait()
    kept = pltpu.make_async_copy(
        wbuf.at[pl.ds(pl.multiple_of(g * r + p * half, half), half), :],
        new_out.at[:, pl.ds(pl.multiple_of(p * cols, cols), cols)], loc.at[1])
    kept.start()

    tok_arrive(1 - p, m)
    tok_start(1 - p, m, ypart, 3)
    tok_start(1 - p, m, sibling, 4)

    def arrive(s, k):
        @pl.when(g - s >= 0)
        def _():
            w_copy(g - s, k, 1).wait_recv()
            send_w(g - s, k)

        @pl.when(g + s < groups)
        def _():
            w_copy(g + s, k, 0).wait_recv()
            send_w(g + s, k)

    def phase(s):
        @pl.loop(0, chunks)
        def _(k):
            arrive(s, k)

    if groups > 2:
        phase(1)
    tok_arrive(p, m_y)
    tok_start(p, m_y, sibling, 5)
    tok_arrive(1 - p, m_y)
    tok_start(1 - p, m_y, sibling, 6)
    if groups > 3:
        @pl.loop(2, groups - 1)
        def _(s):
            phase(s)
    for pp, mm in ((p, m_s), (1 - p, m_s), (p, m_ys), (1 - p, m_ys)):
        tok_arrive(pp, mm)

    def hid_copy(k):
        cc = pl.ds(pl.multiple_of(k * cw, cw), cw)
        oc = pl.ds(pl.multiple_of(p * cols + k * cw, cw), cw)
        return pltpu.make_async_remote_copy(
            src_ref=hid.at[pl.ds(pl.multiple_of(vlm_rows + (1 - p) * act_rows, act_rows), act_rows), cc],
            dst_ref=act_out.at[:, oc], send_sem=hid_send.at[k], recv_sem=hid_recv.at[k],
            device_id=xpart, device_id_type=MESH)

    def hid_back(k):
        oc = pl.ds(pl.multiple_of((1 - p) * cols + k * cw, cw), cw)
        return pltpu.make_async_remote_copy(
            src_ref=act_out.at[:, oc], dst_ref=act_out.at[:, oc], send_sem=hid_send.at[k],
            recv_sem=hid_recv.at[k], device_id=xpart, device_id_type=MESH)

    def own_copies(k):
        cc = pl.ds(pl.multiple_of(k * cw, cw), cw)
        oc = pl.ds(pl.multiple_of(p * cols + k * cw, cw), cw)
        return (
            pltpu.make_async_copy(
                hid.at[pl.ds(pl.multiple_of(vlm_rows + p * act_rows, act_rows), act_rows), cc],
                act_out.at[:, oc], loc.at[2 + 2 * k]),
            pltpu.make_async_copy(hid.at[pl.ds(0, vlm_rows), cc], vlm_out.at[:, cc], loc.at[3 + 2 * k]))

    tile = math.gcd(256, math.gcd(vlm_rows, act_rows))

    def compute(first, count, k):
        cc = pl.ds(pl.multiple_of(k * cw, cw), cw)

        @pl.loop(0, count // tile)
        def _(t):
            rows = pl.ds(pl.multiple_of(first + t * tile, tile), tile)
            pre = jnp.dot(tok[rows, :], wbuf[:, cc], preferred_element_type=jnp.float32)
            hid[rows, cc] = gelu(pre)

    @pl.loop(0, chunks)
    def _(k):
        if groups > 1:
            arrive(groups - 1, k)
        compute(vlm_rows + (1 - p) * act_rows, act_rows, k)
        hid_copy(k).start()
        compute(vlm_rows + p * act_rows, act_rows, k)
        own_copies(k)[0].start()
        compute(0, vlm_rows, k)
        own_copies(k)[1].start()

    to_of = ((p, m, xpart), (p, m, ypart), (p, m, sibling), (1 - p, m, ypart), (1 - p, m, sibling),
             (p, m_y, sibling), (1 - p, m_y, sibling))
    for slot, (pp, mm, to) in enumerate(to_of):
        for copy in tok_copies(pp, mm, to, slot):
            copy.wait_send()

    @pl.loop(0, groups)
    def _(block):
        @pl.loop(0, chunks)
        def _(k):
            @pl.when(has_left & (block >= g))
            def _():
                w_copy(block, k, 0).wait_send()

            @pl.when(has_right & (block <= g))
            def _():
                w_copy(block, k, 1).wait_send()

    ex.wait_send()
    pltpu.make_async_remote_copy(
        src_ref=proj_ref.at[pl.ds(given, half), :],
        dst_ref=new_out.at[:, pl.ds(pl.multiple_of((1 - p) * cols, cols), cols)],
        send_sem=ex_send, recv_sem=ex_recv, device_id=xpart, device_id_type=MESH).wait_recv()
    kept.wait()

    @pl.loop(0, chunks)
    def _(k):
        for copy in own_copies(k):
            copy.wait()
        hid_copy(k).wait_send()
        hid_back(k).wait_recv()


def solution(mesh):
    groups, mp_size = mesh.shape["dp"] // 2, mesh.shape["mp"]

    def local(vlm_tokens, action_tokens, norm_gain, proj_old):
        vr, ar = vlm_tokens.shape[0], action_tokens.shape[0]
        features = vlm_tokens.shape[1]
        r, cols = proj_old.shape
        vlm_rows, act_rows = 2 * mp_size * vr, mp_size * ar
        bf16 = jnp.bfloat16
        dma = pltpu.SemaphoreType.DMA
        vmem, hbm = pl.BlockSpec(memory_space=pltpu.VMEM), pl.BlockSpec(memory_space=pl.ANY)
        return pl.pallas_call(
            functools.partial(kernel, groups, mp_size, CHUNKS),
            name="up_gelu",
            out_shape=(
                jax.ShapeDtypeStruct((vlm_rows, cols), bf16),
                jax.ShapeDtypeStruct((act_rows, 2 * cols), bf16),
                jax.ShapeDtypeStruct((r // 2, 2 * cols), bf16),
            ),
            in_specs=[vmem, vmem, vmem, hbm],
            out_specs=(hbm, hbm, hbm),
            scratch_shapes=[
                pltpu.VMEM((vlm_rows + 2 * act_rows, features), bf16),
                pltpu.VMEM((groups * r, cols), bf16),
                pltpu.VMEM((vlm_rows + 2 * act_rows, cols), bf16),
                dma((7, 2)), dma((2 * mp_size, 2)),
                dma((2, groups, CHUNKS)), dma((groups, CHUNKS)),
                dma, dma, dma((CHUNKS,)), dma((CHUNKS,)), dma((2 + 2 * CHUNKS,)),
            ],
            compiler_params=pltpu.CompilerParams(
                collective_id=0, has_side_effects=True, vmem_limit_bytes=48 * 1024 * 1024),
        )(vlm_tokens, action_tokens, norm_gain.reshape(1, -1), proj_old)

    return jax.shard_map(
        local,
        mesh=mesh,
        in_specs=(P(("dp", "mp"), None), P(("dp", "mp"), None), P(), P("dp", "mp")),
        out_specs=(P("dp", "mp"), P("dp", "mp"), P("dp", "mp")),
        check_vma=False,
    )
```

```python
import functools
import math
import jax
import jax.numpy as jnp
from jax import lax
from jax.experimental import pallas as pl
from jax.experimental.pallas import tpu as pltpu
from jax.sharding import PartitionSpec as P

MESH = pl.DeviceIdType.MESH
epsilon = 1e-06


def column_plan(cols):
    wide = cols // 4
    narrow = max(wide // 2, 128)
    return ((0, wide, 3, 0), (3 * wide, narrow, wide // narrow, 3))


def number_of_chunks(cols):
    return sum(count for _, _, count, _ in column_plan(cols))


def normalize(row_values, norm_gain):
    values = row_values.astype(jnp.float32)
    factor = lax.rsqrt(jnp.mean(values * values, axis=-1, keepdims=True) + epsilon)
    return (values * factor * norm_gain).astype(jnp.bfloat16)


def gelu(u):
    return (u * 0.5 * (1.0 + lax.erf(u * math.sqrt(0.5)))).astype(jnp.bfloat16)


def kernel(groups, mp_size, vlm_hbm, act_hbm, gain_hbm, proj_hbm, vlm_out, act_out, new_out,
           vlm_ref, act_ref, gain_ref, tok, wbuf, hid, tok_send, tok_recv, w_send, w_recv, ex_send, ex_recv, hid_send, hid_recv, loc, load_sem,
           own_sem, vlm_sem):
    d = lax.axis_index("dp")
    m = lax.axis_index("mp")
    g, p = d // 2, d % 2
    y, c = m // 2, m % 2
    vr, ar = vlm_ref.shape[0], act_ref.shape[0]
    r, cols = proj_hbm.shape
    half = r // 2
    plan = column_plan(cols)
    vlm_rows, act_rows = 2 * mp_size * vr, mp_size * ar
    sibling = (d, y * 2 + 1 - c)
    xpart = (g * 2 + 1 - p, m)
    ypart = (d, (1 - y) * 2 + c)
    has_left, has_right = g > 0, g < groups - 1

    barrier = pltpu.get_barrier_semaphore()
    for other in (sibling, xpart, ypart):
        pl.semaphore_signal(barrier, inc=1, device_id=other, device_id_type=MESH)

    @pl.when(has_left)
    def _():
        pl.semaphore_signal(barrier, inc=1, device_id=(d - 2, m), device_id_type=MESH)

    @pl.when(has_right)
    def _():
        pl.semaphore_signal(barrier, inc=1, device_id=(d + 2, m), device_id_type=MESH)

    def load_w():
        return pltpu.make_async_copy(proj_hbm, wbuf.at[pl.ds(pl.multiple_of(g * r, r), r), :], loc.at[0])

    loads = [pltpu.make_async_copy(src, dst, load_sem.at[i]) for i, (src, dst) in enumerate(
        ((gain_hbm, gain_ref), (vlm_hbm, vlm_ref), (act_hbm, act_ref)))]
    load_w().start()
    for load in loads:
        load.start()
    pl.semaphore_wait(barrier, 3 + has_left.astype(jnp.int32) + has_right.astype(jnp.int32))
    load_w().wait()

    def each_chunk(body):
        for first, width, count, base in plan:
            @pl.loop(0, count)
            def _(i):
                body(pl.ds(pl.multiple_of(first + i * width, width), width), base + i)

    def w_copy(block, cc, k, side):
        rows = pl.ds(pl.multiple_of(block * r, r), r)
        return pltpu.make_async_remote_copy(
            src_ref=wbuf.at[rows, cc],
            dst_ref=wbuf.at[rows, cc],
            send_sem=w_send.at[side, block, k],
            recv_sem=w_recv.at[block, k],
            device_id=(d - 2 if side == 0 else d + 2, m),
            device_id_type=MESH,
        )

    def send_w(block, cc, k):
        @pl.when(has_left & (block >= g))
        def _():
            w_copy(block, cc, k, 0).start()

        @pl.when(has_right & (block <= g))
        def _():
            w_copy(block, cc, k, 1).start()

    each_chunk(lambda cc, k: send_w(g, cc, k))
    for load in loads:
        load.wait()

    def place(pp, mm):
        s = pp * mp_size + mm
        return (pl.ds(pl.multiple_of(s * vr, vr), vr), pl.ds(pl.multiple_of(vlm_rows + s * ar, ar), ar), s)

    step = 32

    @pl.loop(0, vr // step)
    def _(i):
        o = pl.multiple_of(i * step, step)
        tok[pl.ds(pl.multiple_of((p * mp_size + m) * vr + o, step), step), :] = normalize(
            vlm_ref[pl.ds(o, step), :], gain_ref[...])

    @pl.loop(0, ar // step)
    def _(i):
        o = pl.multiple_of(i * step, step)
        tok[pl.ds(pl.multiple_of(vlm_rows + (p * mp_size + m) * ar + o, step), step), :] = normalize(
            act_ref[pl.ds(o, step), :], gain_ref[...])

    def tok_copies(pp, mm, to, slot):
        va, aa, s = place(pp, mm)
        return [pltpu.make_async_remote_copy(
            src_ref=tok.at[rows, :], dst_ref=tok.at[rows, :], send_sem=tok_send.at[slot, j],
            recv_sem=tok_recv.at[s, j], device_id=to, device_id_type=MESH)
            for j, rows in enumerate((va, aa))]

    def tok_start(pp, mm, to, slot):
        for copy in tok_copies(pp, mm, to, slot):
            copy.start()

    def tok_arrive(pp, mm):
        for copy in tok_copies(pp, mm, sibling, 0):
            copy.wait_recv()

    m_y = (1 - y) * 2 + c
    m_s = y * 2 + 1 - c
    m_ys = (1 - y) * 2 + 1 - c
    tok_start(p, m, xpart, 0)
    tok_start(p, m, ypart, 1)
    tok_start(p, m, sibling, 2)

    ex = pltpu.make_async_remote_copy(
        src_ref=wbuf.at[pl.ds(pl.multiple_of(g * r + (1 - p) * half, half), half), :],
        dst_ref=new_out.at[:, pl.ds(pl.multiple_of(p * cols, cols), cols)],
        send_sem=ex_send, recv_sem=ex_recv, device_id=xpart, device_id_type=MESH)
    ex.start()
    kept = pltpu.make_async_copy(
        wbuf.at[pl.ds(pl.multiple_of(g * r + p * half, half), half), :],
        new_out.at[:, pl.ds(pl.multiple_of(p * cols, cols), cols)], loc.at[1])
    kept.start()

    tok_arrive(1 - p, m)
    tok_start(1 - p, m, ypart, 3)
    tok_start(1 - p, m, sibling, 4)

    def arrive(s, cc, k):
        @pl.when(g - s >= 0)
        def _():
            w_copy(g - s, cc, k, 1).wait_recv()
            send_w(g - s, cc, k)

        @pl.when(g + s < groups)
        def _():
            w_copy(g + s, cc, k, 0).wait_recv()
            send_w(g + s, cc, k)

    def phase(s):
        each_chunk(lambda cc, k: arrive(s, cc, k))

    if groups > 2:
        phase(1)
    tok_arrive(p, m_y)
    tok_start(p, m_y, sibling, 5)
    tok_arrive(1 - p, m_y)
    tok_start(1 - p, m_y, sibling, 6)
    if groups > 3:
        @pl.loop(2, groups - 1)
        def _(s):
            phase(s)
    for pp, mm in ((p, m_s), (1 - p, m_s), (p, m_ys), (1 - p, m_ys)):
        tok_arrive(pp, mm)

    tile = math.gcd(256, math.gcd(vlm_rows, act_rows))
    a_tiles, v_tiles = act_rows // tile, vlm_rows // tile

    def out_cols(side, cc):
        return pl.ds(pl.multiple_of(side * cols + cc.start, cc.size), cc.size)

    def tile_rows(start):
        return pl.ds(pl.multiple_of(start, tile), tile)

    def hid_copy(cc, k, t):
        return pltpu.make_async_remote_copy(
            src_ref=hid.at[tile_rows(vlm_rows + (1 - p) * act_rows + t * tile), cc],
            dst_ref=act_out.at[tile_rows(t * tile), out_cols(p, cc)],
            send_sem=hid_send.at[k, t], recv_sem=hid_recv.at[k, t], device_id=xpart, device_id_type=MESH)

    def hid_back(cc, k, t):
        there = act_out.at[tile_rows(t * tile), out_cols(1 - p, cc)]
        return pltpu.make_async_remote_copy(
            src_ref=there, dst_ref=there, send_sem=hid_send.at[k, t], recv_sem=hid_recv.at[k, t],
            device_id=xpart, device_id_type=MESH)

    def own_copy(cc, k):
        return pltpu.make_async_copy(
            hid.at[pl.ds(pl.multiple_of(vlm_rows + p * act_rows, act_rows), act_rows), cc],
            act_out.at[:, out_cols(p, cc)], own_sem.at[k])

    def vlm_copy(cc, k):
        return pltpu.make_async_copy(hid.at[pl.ds(0, vlm_rows), cc], vlm_out.at[:, cc], vlm_sem.at[k])

    def compute(cc, k):
        if groups > 1:
            arrive(groups - 1, cc, k)

        @pl.loop(0, 2 * a_tiles + v_tiles)
        def _(t):
            start = jnp.where(
                t < a_tiles, vlm_rows + (1 - p) * act_rows + t * tile,
                jnp.where(t < 2 * a_tiles, vlm_rows + p * act_rows + (t - a_tiles) * tile, (t - 2 * a_tiles) * tile))
            rows = tile_rows(start)
            pre = jnp.dot(tok[rows, :], wbuf[:, cc], preferred_element_type=jnp.float32)
            hid[rows, cc] = gelu(pre)

            @pl.when(t < a_tiles)
            def _():
                hid_copy(cc, k, t).start()

            @pl.when(t == 2 * a_tiles - 1)
            def _():
                own_copy(cc, k).start()

        vlm_copy(cc, k).start()

    each_chunk(compute)

    to_of = ((p, m, xpart), (p, m, ypart), (p, m, sibling), (1 - p, m, ypart), (1 - p, m, sibling),
             (p, m_y, sibling), (1 - p, m_y, sibling))
    for slot, (pp, mm, to) in enumerate(to_of):
        for copy in tok_copies(pp, mm, to, slot):
            copy.wait_send()

    @pl.loop(0, groups)
    def _(block):
        def sent(cc, k):
            @pl.when(has_left & (block >= g))
            def _():
                w_copy(block, cc, k, 0).wait_send()

            @pl.when(has_right & (block <= g))
            def _():
                w_copy(block, cc, k, 1).wait_send()

        each_chunk(sent)

    ex.wait_send()
    taken = new_out.at[:, pl.ds(pl.multiple_of((1 - p) * cols, cols), cols)]
    pltpu.make_async_remote_copy(
        src_ref=taken, dst_ref=taken, send_sem=ex_send, recv_sem=ex_recv,
        device_id=xpart, device_id_type=MESH).wait_recv()
    kept.wait()

    def finish(cc, k):
        own_copy(cc, k).wait()
        vlm_copy(cc, k).wait()

        @pl.loop(0, a_tiles)
        def _(t):
            hid_copy(cc, k, t).wait_send()
            hid_back(cc, k, t).wait_recv()

    each_chunk(finish)


def store(*refs):
    count = (len(refs) - 1) // 2
    copies = [pltpu.make_async_copy(refs[i], refs[count + i], refs[-1].at[i]) for i in range(count)]
    for copy in copies:
        copy.start()
    for copy in copies:
        copy.wait()


def solution(mesh):
    groups, mp_size = mesh.shape["dp"] // 2, mesh.shape["mp"]

    def local(vlm_tokens, action_tokens, norm_gain, proj_old):
        vr, ar = vlm_tokens.shape[0], action_tokens.shape[0]
        features = vlm_tokens.shape[1]
        r, cols = proj_old.shape
        vlm_rows, act_rows = 2 * mp_size * vr, mp_size * ar
        bf16 = jnp.bfloat16
        dma = pltpu.SemaphoreType.DMA
        hbm, anywhere = pl.BlockSpec(memory_space=pltpu.HBM), pl.BlockSpec(memory_space=pl.ANY)
        chunks = number_of_chunks(cols)
        a_tiles = act_rows // math.gcd(256, math.gcd(vlm_rows, act_rows))
        shapes = (
            jax.ShapeDtypeStruct((vlm_rows, cols), bf16),
            jax.ShapeDtypeStruct((act_rows, 2 * cols), bf16),
            jax.ShapeDtypeStruct((r // 2, 2 * cols), bf16),
        )
        results = pl.pallas_call(
            functools.partial(kernel, groups, mp_size),
            name="up_gelu",
            out_shape=shapes,
            in_specs=[hbm] * 4,
            out_specs=(anywhere,) * 3,
            scratch_shapes=[
                pltpu.VMEM((vr, features), bf16),
                pltpu.VMEM((ar, features), bf16),
                pltpu.VMEM((1, features), jnp.float32),
                pltpu.VMEM((vlm_rows + 2 * act_rows, features), bf16),
                pltpu.VMEM((groups * r, cols), bf16),
                pltpu.VMEM((vlm_rows + 2 * act_rows, cols), bf16),
                dma((7, 2)), dma((2 * mp_size, 2)),
                dma((2, groups, chunks)), dma((groups, chunks)),
                dma, dma, dma((chunks, a_tiles)), dma((chunks, a_tiles)), dma((2,)), dma((3,)),
                dma((chunks,)), dma((chunks,)),
            ],
            compiler_params=pltpu.CompilerParams(
                collective_id=0, has_side_effects=True, vmem_limit_bytes=48 * 1024 * 1024),
        )(*[pltpu.with_memory_space_constraint(array, pltpu.HBM) for array in (
            vlm_tokens, action_tokens, norm_gain.reshape(1, -1), proj_old)])
        return pl.pallas_call(
            store,
            name="store",
            out_shape=shapes,
            in_specs=[anywhere] * 3,
            out_specs=(hbm,) * 3,
            scratch_shapes=[dma((3,))],
            compiler_params=pltpu.CompilerParams(vmem_limit_bytes=1024 * 1024),
        )(*results)

    return jax.shard_map(
        local,
        mesh=mesh,
        in_specs=(P(("dp", "mp"), None), P(("dp", "mp"), None), P(), P("dp", "mp")),
        out_specs=(P("dp", "mp"), P("dp", "mp"), P("dp", "mp")),
        check_vma=False,
    )
```

```python
import functools
import math
import jax
import jax.numpy as jnp
from jax import lax
from jax.experimental import pallas as pl
from jax.experimental.pallas import tpu as pltpu
from jax.sharding import PartitionSpec as P

MESH = pl.DeviceIdType.MESH
epsilon = 1e-06


def column_plan(cols):
    wide = cols // 4
    narrow = max(wide // 2, 128)
    return ((0, wide, 3, 0), (3 * wide, narrow, wide // narrow, 3))


def number_of_chunks(cols):
    return sum(count for _, _, count, _ in column_plan(cols))


def normalize(row_values, norm_gain):
    values = row_values.astype(jnp.float32)
    factor = lax.rsqrt(jnp.mean(values * values, axis=-1, keepdims=True) + epsilon)
    return (values * factor * norm_gain).astype(jnp.bfloat16)


def gelu(u):
    return (u * 0.5 * (1.0 + lax.erf(u * math.sqrt(0.5)))).astype(jnp.bfloat16)


def kernel(groups, mp_size, vlm_hbm, act_hbm, gain_hbm, proj_hbm, vlm_out, act_out, new_out,
           vlm_ref, act_ref, gain_ref, tok, wbuf, hid, tok_send, tok_recv, w_send, w_recv, ex_send, ex_recv, hid_send, hid_recv, loc, load_sem,
           own_sem, vlm_sem, loc_w):
    d = lax.axis_index("dp")
    m = lax.axis_index("mp")
    g, p = d // 2, d % 2
    y, c = m // 2, m % 2
    vr, ar = vlm_ref.shape[0], act_ref.shape[0]
    r, cols = proj_hbm.shape
    half = r // 2
    plan = column_plan(cols)
    vlm_rows, act_rows = 2 * mp_size * vr, mp_size * ar
    sibling = (d, y * 2 + 1 - c)
    xpart = (g * 2 + 1 - p, m)
    ypart = (d, (1 - y) * 2 + c)
    has_left, has_right = g > 0, g < groups - 1

    def each_chunk(body, parts=plan):
        for first, width, count, base in parts:
            @pl.loop(0, count)
            def _(i):
                body(pl.ds(pl.multiple_of(first + i * width, width), width), base + i)

    barrier = pltpu.get_barrier_semaphore()

    @pl.when(has_left)
    def _():
        pl.semaphore_signal(barrier, inc=1, device_id=(d - 2, m), device_id_type=MESH)

    @pl.when(has_right)
    def _():
        pl.semaphore_signal(barrier, inc=1, device_id=(d + 2, m), device_id_type=MESH)

    for other in (xpart, ypart, sibling):
        pl.semaphore_signal(barrier, inc=1, device_id=other, device_id_type=MESH)

    def load_w(cc, k):
        return pltpu.make_async_copy(
            proj_hbm.at[:, cc], wbuf.at[pl.ds(pl.multiple_of(g * r, r), r), cc], loc_w.at[k])

    loads = [pltpu.make_async_copy(src, dst, load_sem.at[i]) for i, (src, dst) in enumerate(
        ((gain_hbm, gain_ref), (vlm_hbm, vlm_ref), (act_hbm, act_ref)))]
    each_chunk(lambda cc, k: load_w(cc, k).start())
    for load in loads:
        load.start()
    pl.semaphore_wait(barrier, 3 + has_left.astype(jnp.int32) + has_right.astype(jnp.int32))

    def w_copy(block, cc, k, side):
        rows = pl.ds(pl.multiple_of(block * r, r), r)
        return pltpu.make_async_remote_copy(
            src_ref=wbuf.at[rows, cc],
            dst_ref=wbuf.at[rows, cc],
            send_sem=w_send.at[side, block, k],
            recv_sem=w_recv.at[block, k],
            device_id=(d - 2 if side == 0 else d + 2, m),
            device_id_type=MESH,
        )

    def send_w(block, cc, k):
        @pl.when(has_left & (block >= g))
        def _():
            w_copy(block, cc, k, 0).start()

        @pl.when(has_right & (block <= g))
        def _():
            w_copy(block, cc, k, 1).start()

    def send_own(cc, k):
        load_w(cc, k).wait()
        send_w(g, cc, k)

    each_chunk(send_own)
    for load in loads:
        load.wait()

    def place(pp, mm):
        s = pp * mp_size + mm
        return (pl.ds(pl.multiple_of(s * vr, vr), vr), pl.ds(pl.multiple_of(vlm_rows + s * ar, ar), ar), s)

    step = 32

    @pl.loop(0, vr // step)
    def _(i):
        o = pl.multiple_of(i * step, step)
        tok[pl.ds(pl.multiple_of((p * mp_size + m) * vr + o, step), step), :] = normalize(
            vlm_ref[pl.ds(o, step), :], gain_ref[...])

    @pl.loop(0, ar // step)
    def _(i):
        o = pl.multiple_of(i * step, step)
        tok[pl.ds(pl.multiple_of(vlm_rows + (p * mp_size + m) * ar + o, step), step), :] = normalize(
            act_ref[pl.ds(o, step), :], gain_ref[...])

    def tok_copies(pp, mm, to, slot):
        va, aa, s = place(pp, mm)
        return [pltpu.make_async_remote_copy(
            src_ref=tok.at[rows, :], dst_ref=tok.at[rows, :], send_sem=tok_send.at[slot, j],
            recv_sem=tok_recv.at[s, j], device_id=to, device_id_type=MESH)
            for j, rows in enumerate((va, aa))]

    def tok_start(pp, mm, to, slot):
        for copy in tok_copies(pp, mm, to, slot):
            copy.start()

    def tok_arrive(pp, mm):
        for copy in tok_copies(pp, mm, sibling, 0):
            copy.wait_recv()

    m_y = (1 - y) * 2 + c
    m_s = y * 2 + 1 - c
    m_ys = (1 - y) * 2 + 1 - c
    tok_start(p, m, xpart, 0)
    tok_start(p, m, ypart, 1)
    tok_start(p, m, sibling, 2)

    ex = pltpu.make_async_remote_copy(
        src_ref=wbuf.at[pl.ds(pl.multiple_of(g * r + (1 - p) * half, half), half), :],
        dst_ref=new_out.at[:, pl.ds(pl.multiple_of(p * cols, cols), cols)],
        send_sem=ex_send, recv_sem=ex_recv, device_id=xpart, device_id_type=MESH)
    ex.start()
    kept = pltpu.make_async_copy(
        wbuf.at[pl.ds(pl.multiple_of(g * r + p * half, half), half), :],
        new_out.at[:, pl.ds(pl.multiple_of(p * cols, cols), cols)], loc)
    kept.start()

    def arrive(s, cc, k):
        @pl.when(g - s >= 0)
        def _():
            w_copy(g - s, cc, k, 1).wait_recv()
            send_w(g - s, cc, k)

        @pl.when(g + s < groups)
        def _():
            w_copy(g + s, cc, k, 0).wait_recv()
            send_w(g + s, cc, k)

    def phase(s, parts=plan):
        each_chunk(lambda cc, k: arrive(s, cc, k), parts)

    if groups > 2:
        phase(1, plan[:1])
    tok_arrive(1 - p, m)
    tok_start(1 - p, m, ypart, 3)
    tok_start(1 - p, m, sibling, 4)
    if groups > 2:
        phase(1, plan[1:])
    tok_arrive(p, m_y)
    tok_start(p, m_y, sibling, 5)
    tok_arrive(1 - p, m_y)
    tok_start(1 - p, m_y, sibling, 6)
    if groups > 3:
        @pl.loop(2, groups - 1)
        def _(s):
            phase(s)
    for pp, mm in ((p, m_s), (1 - p, m_s), (p, m_ys), (1 - p, m_ys)):
        tok_arrive(pp, mm)

    tile = math.gcd(256, math.gcd(vlm_rows, act_rows))
    a_tiles, v_tiles = act_rows // tile, vlm_rows // tile

    def out_cols(side, cc):
        return pl.ds(pl.multiple_of(side * cols + cc.start, cc.size), cc.size)

    def tile_rows(start):
        return pl.ds(pl.multiple_of(start, tile), tile)

    def hid_copy(cc, k, t):
        return pltpu.make_async_remote_copy(
            src_ref=hid.at[tile_rows(vlm_rows + (1 - p) * act_rows + t * tile), cc],
            dst_ref=act_out.at[tile_rows(t * tile), out_cols(p, cc)],
            send_sem=hid_send.at[k, t], recv_sem=hid_recv.at[k, t], device_id=xpart, device_id_type=MESH)

    def hid_back(cc, k, t):
        there = act_out.at[tile_rows(t * tile), out_cols(1 - p, cc)]
        return pltpu.make_async_remote_copy(
            src_ref=there, dst_ref=there, send_sem=hid_send.at[k, t], recv_sem=hid_recv.at[k, t],
            device_id=xpart, device_id_type=MESH)

    def own_copy(cc, k):
        return pltpu.make_async_copy(
            hid.at[pl.ds(pl.multiple_of(vlm_rows + p * act_rows, act_rows), act_rows), cc],
            act_out.at[:, out_cols(p, cc)], own_sem.at[k])

    def vlm_copy(cc, k):
        return pltpu.make_async_copy(hid.at[pl.ds(0, vlm_rows), cc], vlm_out.at[:, cc], vlm_sem.at[k])

    def compute(cc, k):
        if groups > 1:
            arrive(groups - 1, cc, k)

        @pl.loop(0, 2 * a_tiles + v_tiles)
        def _(t):
            start = jnp.where(
                t < a_tiles, vlm_rows + (1 - p) * act_rows + t * tile,
                jnp.where(t < 2 * a_tiles, vlm_rows + p * act_rows + (t - a_tiles) * tile, (t - 2 * a_tiles) * tile))
            rows = tile_rows(start)
            pre = jnp.dot(tok[rows, :], wbuf[:, cc], preferred_element_type=jnp.float32)
            hid[rows, cc] = gelu(pre)

            @pl.when(t < a_tiles)
            def _():
                hid_copy(cc, k, t).start()

            @pl.when(t == 2 * a_tiles - 1)
            def _():
                own_copy(cc, k).start()

        vlm_copy(cc, k).start()

    each_chunk(compute)

    to_of = ((p, m, xpart), (p, m, ypart), (p, m, sibling), (1 - p, m, ypart), (1 - p, m, sibling),
             (p, m_y, sibling), (1 - p, m_y, sibling))
    for slot, (pp, mm, to) in enumerate(to_of):
        for copy in tok_copies(pp, mm, to, slot):
            copy.wait_send()

    @pl.loop(0, groups)
    def _(block):
        def sent(cc, k):
            @pl.when(has_left & (block >= g))
            def _():
                w_copy(block, cc, k, 0).wait_send()

            @pl.when(has_right & (block <= g))
            def _():
                w_copy(block, cc, k, 1).wait_send()

        each_chunk(sent)

    ex.wait_send()
    taken = new_out.at[:, pl.ds(pl.multiple_of((1 - p) * cols, cols), cols)]
    pltpu.make_async_remote_copy(
        src_ref=taken, dst_ref=taken, send_sem=ex_send, recv_sem=ex_recv,
        device_id=xpart, device_id_type=MESH).wait_recv()
    kept.wait()

    def finish(cc, k):
        own_copy(cc, k).wait()
        vlm_copy(cc, k).wait()

        @pl.loop(0, a_tiles)
        def _(t):
            hid_copy(cc, k, t).wait_send()
            hid_back(cc, k, t).wait_recv()

    each_chunk(finish)


def store(*refs):
    count = (len(refs) - 1) // 2
    copies = [pltpu.make_async_copy(refs[i], refs[count + i], refs[-1].at[i]) for i in range(count)]
    for copy in copies:
        copy.start()
    for copy in copies:
        copy.wait()


def solution(mesh):
    groups, mp_size = mesh.shape["dp"] // 2, mesh.shape["mp"]

    def local(vlm_tokens, action_tokens, norm_gain, proj_old):
        vr, ar = vlm_tokens.shape[0], action_tokens.shape[0]
        features = vlm_tokens.shape[1]
        r, cols = proj_old.shape
        vlm_rows, act_rows = 2 * mp_size * vr, mp_size * ar
        bf16 = jnp.bfloat16
        dma = pltpu.SemaphoreType.DMA
        hbm, anywhere = pl.BlockSpec(memory_space=pltpu.HBM), pl.BlockSpec(memory_space=pl.ANY)
        chunks = number_of_chunks(cols)
        a_tiles = act_rows // math.gcd(256, math.gcd(vlm_rows, act_rows))
        shapes = (
            jax.ShapeDtypeStruct((vlm_rows, cols), bf16),
            jax.ShapeDtypeStruct((act_rows, 2 * cols), bf16),
            jax.ShapeDtypeStruct((r // 2, 2 * cols), bf16),
        )
        results = pl.pallas_call(
            functools.partial(kernel, groups, mp_size),
            name="up_gelu",
            out_shape=shapes,
            in_specs=[hbm] * 4,
            out_specs=(anywhere,) * 3,
            scratch_shapes=[
                pltpu.VMEM((vr, features), bf16),
                pltpu.VMEM((ar, features), bf16),
                pltpu.VMEM((1, features), jnp.float32),
                pltpu.VMEM((vlm_rows + 2 * act_rows, features), bf16),
                pltpu.VMEM((groups * r, cols), bf16),
                pltpu.VMEM((vlm_rows + 2 * act_rows, cols), bf16),
                dma((7, 2)), dma((2 * mp_size, 2)),
                dma((2, groups, chunks)), dma((groups, chunks)),
                dma, dma, dma((chunks, a_tiles)), dma((chunks, a_tiles)), dma, dma((3,)),
                dma((chunks,)), dma((chunks,)), dma((chunks,)),
            ],
            compiler_params=pltpu.CompilerParams(
                collective_id=0, has_side_effects=True, vmem_limit_bytes=48 * 1024 * 1024),
        )(*[pltpu.with_memory_space_constraint(array, pltpu.HBM) for array in (
            vlm_tokens, action_tokens, norm_gain.reshape(1, -1), proj_old)])
        return pl.pallas_call(
            store,
            name="store",
            out_shape=shapes,
            in_specs=[anywhere] * 3,
            out_specs=(hbm,) * 3,
            scratch_shapes=[dma((3,))],
            compiler_params=pltpu.CompilerParams(vmem_limit_bytes=1024 * 1024),
        )(*results)

    return jax.shard_map(
        local,
        mesh=mesh,
        in_specs=(P(("dp", "mp"), None), P(("dp", "mp"), None), P(), P("dp", "mp")),
        out_specs=(P("dp", "mp"), P("dp", "mp"), P("dp", "mp")),
        check_vma=False,
    )
```

```python
import functools
import math
import jax
import jax.numpy as jnp
from jax import lax
from jax.experimental import pallas as pl
from jax.experimental.pallas import tpu as pltpu
from jax.sharding import PartitionSpec as P

MESH = pl.DeviceIdType.MESH
epsilon = 1e-06


def column_plan(cols):
    wide = cols // 4
    narrow = max(wide // 2, 128)
    return ((0, wide, 3, 0), (3 * wide, narrow, wide // narrow, 3))


def number_of_chunks(cols):
    return sum(count for _, _, count, _ in column_plan(cols))


def normalize(row_values, norm_gain):
    values = row_values.astype(jnp.float32)
    factor = lax.rsqrt(jnp.mean(values * values, axis=-1, keepdims=True) + epsilon)
    return (values * factor * norm_gain).astype(jnp.bfloat16)


def gelu(u):
    return (u * 0.5 * (1.0 + lax.erf(u * math.sqrt(0.5)))).astype(jnp.bfloat16)


def kernel(groups, mp_size, vlm_hbm, act_hbm, gain_hbm, proj_hbm, vlm_out, act_out, new_out,
           vlm_ref, act_ref, gain_ref, tok, wbuf, hid, tok_send, tok_recv, w_send, w_recv, ex_send, ex_recv, hid_send, hid_recv, loc, load_sem,
           own_sem, vlm_sem, loc_w):
    d = lax.axis_index("dp")
    m = lax.axis_index("mp")
    g, p = d // 2, d % 2
    y, c = m // 2, m % 2
    vr, ar = vlm_ref.shape[0], act_ref.shape[0]
    r, cols = proj_hbm.shape
    half = r // 2
    plan = column_plan(cols)
    vlm_rows, act_rows = 2 * mp_size * vr, mp_size * ar
    sibling = (d, y * 2 + 1 - c)
    xpart = (g * 2 + 1 - p, m)
    ypart = (d, (1 - y) * 2 + c)
    has_left, has_right = g > 0, g < groups - 1

    def each_chunk(body, parts=plan):
        for first, width, count, base in parts:
            @pl.loop(0, count)
            def _(i):
                body(pl.ds(pl.multiple_of(first + i * width, width), width), base + i)

    barrier = pltpu.get_barrier_semaphore()

    @pl.when(has_left)
    def _():
        pl.semaphore_signal(barrier, inc=1, device_id=(d - 2, m), device_id_type=MESH)

    @pl.when(has_right)
    def _():
        pl.semaphore_signal(barrier, inc=1, device_id=(d + 2, m), device_id_type=MESH)

    for other in (xpart, ypart, sibling):
        pl.semaphore_signal(barrier, inc=1, device_id=other, device_id_type=MESH)

    def load_w(cc, k):
        return pltpu.make_async_copy(
            proj_hbm.at[:, cc], wbuf.at[pl.ds(pl.multiple_of(g * r, r), r), cc], loc_w.at[k])

    loads = [pltpu.make_async_copy(src, dst, load_sem.at[i]) for i, (src, dst) in enumerate(
        ((gain_hbm, gain_ref), (vlm_hbm, vlm_ref), (act_hbm, act_ref)))]
    each_chunk(lambda cc, k: load_w(cc, k).start())
    for load in loads:
        load.start()
    pl.semaphore_wait(barrier, 3 + has_left.astype(jnp.int32) + has_right.astype(jnp.int32))

    def w_copy(block, cc, k, side):
        rows = pl.ds(pl.multiple_of(block * r, r), r)
        return pltpu.make_async_remote_copy(
            src_ref=wbuf.at[rows, cc],
            dst_ref=wbuf.at[rows, cc],
            send_sem=w_send.at[side, block, k],
            recv_sem=w_recv.at[block, k],
            device_id=(d - 2 if side == 0 else d + 2, m),
            device_id_type=MESH,
        )

    def send_w(block, cc, k):
        @pl.when(has_left & (block >= g))
        def _():
            w_copy(block, cc, k, 0).start()

        @pl.when(has_right & (block <= g))
        def _():
            w_copy(block, cc, k, 1).start()

    def send_own(cc, k):
        load_w(cc, k).wait()
        send_w(g, cc, k)

    each_chunk(send_own)
    for load in loads:
        load.wait()

    def place(pp, mm):
        s = pp * mp_size + mm
        return (pl.ds(pl.multiple_of(s * vr, vr), vr), pl.ds(pl.multiple_of(vlm_rows + s * ar, ar), ar), s)

    step = 32

    @pl.loop(0, vr // step)
    def _(i):
        o = pl.multiple_of(i * step, step)
        tok[pl.ds(pl.multiple_of((p * mp_size + m) * vr + o, step), step), :] = normalize(
            vlm_ref[pl.ds(o, step), :], gain_ref[...])

    @pl.loop(0, ar // step)
    def _(i):
        o = pl.multiple_of(i * step, step)
        tok[pl.ds(pl.multiple_of(vlm_rows + (p * mp_size + m) * ar + o, step), step), :] = normalize(
            act_ref[pl.ds(o, step), :], gain_ref[...])

    def tok_copies(pp, mm, to, slot):
        va, aa, s = place(pp, mm)
        return [pltpu.make_async_remote_copy(
            src_ref=tok.at[rows, :], dst_ref=tok.at[rows, :], send_sem=tok_send.at[slot, j],
            recv_sem=tok_recv.at[s, j], device_id=to, device_id_type=MESH)
            for j, rows in enumerate((va, aa))]

    def tok_start(pp, mm, to, slot):
        for copy in tok_copies(pp, mm, to, slot):
            copy.start()

    def tok_arrive(pp, mm):
        for copy in tok_copies(pp, mm, sibling, 0):
            copy.wait_recv()

    m_y = (1 - y) * 2 + c
    m_s = y * 2 + 1 - c
    m_ys = (1 - y) * 2 + 1 - c
    tok_start(p, m, xpart, 0)
    tok_start(p, m, ypart, 1)
    tok_start(p, m, sibling, 2)

    ex = pltpu.make_async_remote_copy(
        src_ref=wbuf.at[pl.ds(pl.multiple_of(g * r + (1 - p) * half, half), half), :],
        dst_ref=new_out.at[:, pl.ds(pl.multiple_of(p * cols, cols), cols)],
        send_sem=ex_send, recv_sem=ex_recv, device_id=xpart, device_id_type=MESH)
    ex.start()
    kept = pltpu.make_async_copy(
        wbuf.at[pl.ds(pl.multiple_of(g * r + p * half, half), half), :],
        new_out.at[:, pl.ds(pl.multiple_of(p * cols, cols), cols)], loc)
    kept.start()

    def arrive(s, cc, k):
        @pl.when(g - s >= 0)
        def _():
            w_copy(g - s, cc, k, 1).wait_recv()
            send_w(g - s, cc, k)

        @pl.when(g + s < groups)
        def _():
            w_copy(g + s, cc, k, 0).wait_recv()
            send_w(g + s, cc, k)

    def phase(s, parts=plan):
        each_chunk(lambda cc, k: arrive(s, cc, k), parts)

    if groups > 2:
        phase(1, plan[:1])
    tok_arrive(1 - p, m)
    tok_start(1 - p, m, ypart, 3)
    tok_start(1 - p, m, sibling, 4)
    if groups > 2:
        phase(1, plan[1:])
    tok_arrive(p, m_y)
    tok_start(p, m_y, sibling, 5)
    tok_arrive(1 - p, m_y)
    tok_start(1 - p, m_y, sibling, 6)
    if groups > 3:
        @pl.loop(2, groups - 1)
        def _(s):
            phase(s)
    for pp, mm in ((p, m_s), (1 - p, m_s), (p, m_ys), (1 - p, m_ys)):
        tok_arrive(pp, mm)

    tile = math.gcd(256, math.gcd(vlm_rows, act_rows))
    a_tiles, v_tiles = act_rows // tile, vlm_rows // tile

    def out_cols(side, cc):
        return pl.ds(pl.multiple_of(side * cols + cc.start, cc.size), cc.size)

    def tile_rows(start):
        return pl.ds(pl.multiple_of(start, tile), tile)

    def hid_copy(cc, k, t):
        return pltpu.make_async_remote_copy(
            src_ref=hid.at[tile_rows(vlm_rows + (1 - p) * act_rows + t * tile), cc],
            dst_ref=act_out.at[tile_rows(t * tile), out_cols(p, cc)],
            send_sem=hid_send.at[k, t], recv_sem=hid_recv.at[k, t], device_id=xpart, device_id_type=MESH)

    def hid_back(cc, k, t):
        there = act_out.at[tile_rows(t * tile), out_cols(1 - p, cc)]
        return pltpu.make_async_remote_copy(
            src_ref=there, dst_ref=there, send_sem=hid_send.at[k, t], recv_sem=hid_recv.at[k, t],
            device_id=xpart, device_id_type=MESH)

    def own_copy(cc, k):
        return pltpu.make_async_copy(
            hid.at[pl.ds(pl.multiple_of(vlm_rows + p * act_rows, act_rows), act_rows), cc],
            act_out.at[:, out_cols(p, cc)], own_sem.at[k])

    def vlm_copy(cc, k):
        return pltpu.make_async_copy(hid.at[pl.ds(0, vlm_rows), cc], vlm_out.at[:, cc], vlm_sem.at[k])

    def hidden(rows, cc):
        pre = jnp.dot(tok[rows, :], wbuf[:, cc], preferred_element_type=jnp.float32)
        hid[rows, cc] = gelu(pre)

    def for_partner(cc, k):
        if groups > 1:
            arrive(groups - 1, cc, k)

        @pl.loop(0, a_tiles)
        def _(t):
            hidden(tile_rows(vlm_rows + (1 - p) * act_rows + t * tile), cc)
            hid_copy(cc, k, t).start()

    def for_self(cc, k):
        @pl.loop(0, a_tiles + v_tiles)
        def _(t):
            hidden(tile_rows(jnp.where(
                t < a_tiles, vlm_rows + p * act_rows + t * tile, (t - a_tiles) * tile)), cc)

            @pl.when(t == a_tiles - 1)
            def _():
                own_copy(cc, k).start()

        vlm_copy(cc, k).start()

    def for_both(cc, k):
        for_partner(cc, k)
        for_self(cc, k)

    first, width, count, base = plan[1]
    merged = ((first, width * count, 1, base),)
    each_chunk(for_both, plan[:1])
    each_chunk(for_partner, plan[1:])
    each_chunk(for_self, merged)

    to_of = ((p, m, xpart), (p, m, ypart), (p, m, sibling), (1 - p, m, ypart), (1 - p, m, sibling),
             (p, m_y, sibling), (1 - p, m_y, sibling))
    for slot, (pp, mm, to) in enumerate(to_of):
        for copy in tok_copies(pp, mm, to, slot):
            copy.wait_send()

    @pl.loop(0, groups)
    def _(block):
        def sent(cc, k):
            @pl.when(has_left & (block >= g))
            def _():
                w_copy(block, cc, k, 0).wait_send()

            @pl.when(has_right & (block <= g))
            def _():
                w_copy(block, cc, k, 1).wait_send()

        each_chunk(sent)

    ex.wait_send()
    taken = new_out.at[:, pl.ds(pl.multiple_of((1 - p) * cols, cols), cols)]
    pltpu.make_async_remote_copy(
        src_ref=taken, dst_ref=taken, send_sem=ex_send, recv_sem=ex_recv,
        device_id=xpart, device_id_type=MESH).wait_recv()
    kept.wait()

    def finish(cc, k):
        @pl.loop(0, a_tiles)
        def _(t):
            hid_copy(cc, k, t).wait_send()
            hid_back(cc, k, t).wait_recv()

    def stored(cc, k):
        own_copy(cc, k).wait()
        vlm_copy(cc, k).wait()

    each_chunk(stored, plan[:1] + merged)
    each_chunk(finish)


def store(*refs):
    count = (len(refs) - 1) // 2
    copies = [pltpu.make_async_copy(refs[i], refs[count + i], refs[-1].at[i]) for i in range(count)]
    for copy in copies:
        copy.start()
    for copy in copies:
        copy.wait()


def solution(mesh):
    groups, mp_size = mesh.shape["dp"] // 2, mesh.shape["mp"]

    def local(vlm_tokens, action_tokens, norm_gain, proj_old):
        vr, ar = vlm_tokens.shape[0], action_tokens.shape[0]
        features = vlm_tokens.shape[1]
        r, cols = proj_old.shape
        vlm_rows, act_rows = 2 * mp_size * vr, mp_size * ar
        bf16 = jnp.bfloat16
        dma = pltpu.SemaphoreType.DMA
        hbm, anywhere = pl.BlockSpec(memory_space=pltpu.HBM), pl.BlockSpec(memory_space=pl.ANY)
        chunks = number_of_chunks(cols)
        a_tiles = act_rows // math.gcd(256, math.gcd(vlm_rows, act_rows))
        shapes = (
            jax.ShapeDtypeStruct((vlm_rows, cols), bf16),
            jax.ShapeDtypeStruct((act_rows, 2 * cols), bf16),
            jax.ShapeDtypeStruct((r // 2, 2 * cols), bf16),
        )
        results = pl.pallas_call(
            functools.partial(kernel, groups, mp_size),
            name="up_gelu",
            out_shape=shapes,
            in_specs=[hbm] * 4,
            out_specs=(anywhere,) * 3,
            scratch_shapes=[
                pltpu.VMEM((vr, features), bf16),
                pltpu.VMEM((ar, features), bf16),
                pltpu.VMEM((1, features), jnp.float32),
                pltpu.VMEM((vlm_rows + 2 * act_rows, features), bf16),
                pltpu.VMEM((groups * r, cols), bf16),
                pltpu.VMEM((vlm_rows + 2 * act_rows, cols), bf16),
                dma((7, 2)), dma((2 * mp_size, 2)),
                dma((2, groups, chunks)), dma((groups, chunks)),
                dma, dma, dma((chunks, a_tiles)), dma((chunks, a_tiles)), dma, dma((3,)),
                dma((chunks,)), dma((chunks,)), dma((chunks,)),
            ],
            compiler_params=pltpu.CompilerParams(
                collective_id=0, has_side_effects=True, vmem_limit_bytes=48 * 1024 * 1024),
        )(*[pltpu.with_memory_space_constraint(array, pltpu.HBM) for array in (
            vlm_tokens, action_tokens, norm_gain.reshape(1, -1), proj_old)])
        return pl.pallas_call(
            store,
            name="store",
            out_shape=shapes,
            in_specs=[anywhere] * 3,
            out_specs=(hbm,) * 3,
            scratch_shapes=[dma((3,))],
            compiler_params=pltpu.CompilerParams(vmem_limit_bytes=1024 * 1024),
        )(*results)

    return jax.shard_map(
        local,
        mesh=mesh,
        in_specs=(P(("dp", "mp"), None), P(("dp", "mp"), None), P(), P("dp", "mp")),
        out_specs=(P("dp", "mp"), P("dp", "mp"), P("dp", "mp")),
        check_vma=False,
    )
```
